32 devices in a mesh: dp: 4 (over y, core), expert: 8 (over z, x).
Axes of the slice: x: 2, y: 2, z: 4, core: 2. Of those that a mesh axis runs over, the one named last changes fastest.
Arguments:
- hidden: bfloat16 [8192, 768], P(('dp', 'expert')), may hold values from -6 to 6
- w_down: bfloat16 [8, 768, 2048], P('expert', 'dp'), may hold values from -0.21875 to 0.21875
- expert_ids: int32 [1024, 4], P(('dp', 'expert')), may hold values from 0 to 7, all different within a row; in each aligned block of 32 rows (0 to 31, 32 to 63, ...) at most 32 rows name the same one
- gates: float32 [1024, 4], P(('dp', 'expert')), may hold values from 0.05 to 1
- cotangent: bfloat16 [1024, 2048], P(('dp', 'expert')), may hold values from -6 to 6
Outputs:
- mixed: bfloat16 [1024, 2048], P(('dp', 'expert'))
- gate_grads: float32 [1024, 4], P(('dp', 'expert'))
- hidden_grads: bfloat16 [8192, 768], P(('dp', 'expert'))
- weight_grads: bfloat16 [8, 768, 2048], P('expert', 'dp')
The draws below stay inside these ranges and needn't reach their ends.
Inputs may be any that keep to these rules, and one draw needn't show every extreme that they name: `expert_ids`: each row names 4 different experts. Among the rows of one device no expert is named more than 32 times, a bound that some block reaches.
All inputs are finite; a program needn't handle non-finite values.
Results may differ from the reference program's by a relative error of at most 0.015.
Values may be sent and summed in bfloat16 or wider, within the bound.
A program may use at most 64 MiB of HBM per device.

```python
import math
import jax
import jax.numpy as jnp
import numpy as np
from jax import lax

D = 2048
F = 768
TOPK = 4
TOK_DEV = 32
CAP = 32
RECV = 256
EXPERTS = 8
TOKENS = 1024
N_DP = 4
N_EXPERT = 8


def level_of(rng, dims, shards, smallest, high):
    loudness, own = 1.0, jax.random.fold_in(rng, 6)
    for dim, shards_of in shards:
        heights = jnp.exp(jax.random.uniform(jax.random.fold_in(own, dim), (shards_of,), jnp.float32, smallest / len(shards), high / len(shards)))
        loudness = loudness * jnp.repeat(heights, dims[dim] // shards_of).reshape([-1 if axis == dim else 1 for axis in range(len(dims))])
    return loudness


def assign_block(stream_key, own, number, rows, amount, top, reach, slope):
    ranking = jax.random.permutation(stream_key, amount)
    crowded, common = shares(amount, rows * top, reach, slope, True), shares(amount, rows * top, reach, slope, False)
    places = jnp.arange(amount)

    def named(lengths, offset_by):
        used = int((lengths > 0).sum())
        fixed = max(1, used // 4)
        shifted = fixed + (places - fixed + offset_by * (used - fixed)) % max(1, amount - fixed)
        return jnp.zeros((amount,), jnp.int32).at[ranking[jnp.where(places < fixed, places, shifted)]].set(jnp.asarray(lengths, jnp.int32))

    lengths = jnp.where(number % 4 == 0, named(crowded, number // 4), named(common, number - number // 4 - 1))
    mixed = jax.random.permutation(jax.random.fold_in(own, 3), amount)
    giver, receiver = mixed[0:amount // 2 * 2:2], mixed[1:amount // 2 * 2:2]
    room = jnp.minimum(lengths[giver] - 1, reach - lengths[receiver]) // 2
    room = jnp.where((giver == ranking[0]) | (receiver == ranking[0]) | (lengths[receiver] == 0), 0, jnp.maximum(room, 0))
    shifted = jax.random.randint(jax.random.fold_in(own, 4), (amount // 2,), 0, 1 << 20) % (room + 1)
    lengths = lengths.at[giver].add(-shifted).at[receiver].add(shifted)
    labels = jnp.searchsorted(jnp.cumsum(lengths), jnp.arange(rows * top), side="right").astype(jnp.int32)
    table = labels.reshape(top, rows).T
    table = table[jax.random.permutation(jax.random.fold_in(own, 1), rows)]
    offset_by = jax.random.randint(jax.random.fold_in(own, 2), (rows, 1), 0, top)
    return jnp.take_along_axis(table, (jnp.arange(top)[None, :] + offset_by) % top, axis=1)


def shares(amount, total, bound, slope, full):
    portions = [(1 << 20) // math.isqrt(grade ** slope) + 1 for grade in range(1, amount + 1)]
    largest = bound if full else min(bound, max(-(-total // amount), total * portions[0] // sum(portions)))
    least = 1 if total - largest >= amount - 1 else 0
    holding, spare = [largest] + [least] * (amount - 1), total - largest - least * (amount - 1)
    while spare > 0:
        movable = [i for i in range(1, amount) if holding[i] < largest] or [i for i in range(1, amount) if holding[i] < bound]
        mass, left = sum([portions[i] for i in movable]), spare
        for i in movable:
            extra = min(bound - holding[i], max(1, left * portions[i] // mass), spare)
            holding[i] = holding[i] + extra
            spare = spare - extra
    return np.array(holding)


def bell_draw(own_key, shape, deviation, limit, cuts=(), kind=jnp.bfloat16):
    factor_of = level_of(own_key, shape, cuts, -0.22, 0.18) if cuts else 1.0
    result = jax.random.normal(own_key, shape, jnp.float32) * deviation * factor_of
    return jnp.minimum(jnp.maximum(result, -limit), limit).astype(kind)


def setup_inputs(seed: int = 0) -> dict:
    splits = jax.random.split(jax.random.key(seed), 6)
    hidden = bell_draw(splits[0], (N_DP * N_EXPERT * RECV, F), 1.0, 6.0, ((0, 32),))
    w_down = bell_draw(splits[1], (EXPERTS, F, D), F ** -0.5, 0.21875, ((0, 8), (1, 4)))
    expert_ids_keys = jax.random.split(jax.random.fold_in(splits[2], 1), TOKENS // TOK_DEV)
    expert_ids_turns = jax.random.permutation(jax.random.fold_in(splits[2], 3), TOKENS // TOK_DEV)
    expert_ids = jax.vmap(lambda own, number: assign_block(jax.random.fold_in(splits[2], 2), own, number, TOK_DEV, N_EXPERT, TOPK, CAP, 2))(expert_ids_keys, expert_ids_turns).reshape((TOKENS, TOPK))
    gates = jnp.clip(jnp.exp(math.log(1.0) - 2.9957323 * jax.random.uniform(splits[3], (TOKENS, TOPK), jnp.float32) ** level_of(splits[3], (TOKENS, TOPK), ((0, 32),), -0.2, 0.2)), 0.05, 1.0)
    cotangent = bell_draw(splits[4], (TOKENS, D), 1.0, 6.0, ((0, 32),))
    return {"hidden": hidden, "w_down": w_down, "expert_ids": expert_ids, "gates": gates, "cotangent": cotangent}


def positions(flat_ids):
    choose = (flat_ids[:, None] == jnp.arange(N_EXPERT, dtype=jnp.int32)[None, :]).astype(jnp.int32)
    earlier = jnp.cumsum(choose, axis=0) - choose
    return jnp.sum(earlier * choose, axis=1).astype(jnp.int32)


def reference(hidden, w_down, expert_ids, gates, cotangent):
    h_all = hidden.reshape(N_DP, N_EXPERT, N_EXPERT, CAP, F)
    id_all = expert_ids.reshape(N_DP, N_EXPERT, TOK_DEV, TOPK)
    gate_all = gates.reshape(N_DP, N_EXPERT, TOK_DEV, TOPK)
    cot_all = cotangent.reshape(N_DP, N_EXPERT, TOK_DEV, D)
    weight32 = w_down.astype(jnp.float32)
    senders = jnp.arange(N_EXPERT, dtype=jnp.int32)[:, None]
    highest = lax.Precision.HIGHEST

    def one_row(total, pieces):
        h_row, id_row, gate_row, cot_row = pieces
        h32 = h_row.astype(jnp.float32)
        outputs = jnp.einsum("ebcf,efd->ebcd", h32, weight32, precision=highest).astype(jnp.bfloat16)
        flat_ids = id_row.reshape(N_EXPERT, TOK_DEV * TOPK)
        position = jax.vmap(positions)(flat_ids)
        sender_ids = jnp.broadcast_to(senders, flat_ids.shape)
        picked = outputs[flat_ids, sender_ids, position].astype(jnp.float32).reshape(N_EXPERT, TOK_DEV, TOPK, D)
        cot32 = cot_row.astype(jnp.float32)
        mixed = jnp.sum(gate_row[..., None] * picked, axis=2).astype(jnp.bfloat16)
        gate_grads = jnp.sum(picked * cot32[:, :, None, :], axis=3)
        routed = (gate_row[..., None] * cot32[:, :, None, :]).astype(jnp.bfloat16).reshape(N_EXPERT, TOK_DEV * TOPK, D)
        grads_in = jnp.zeros((N_EXPERT, N_EXPERT, CAP, D), jnp.bfloat16).at[flat_ids, sender_ids, position].set(routed)
        grads32 = grads_in.astype(jnp.float32)
        hidden_grads = jnp.einsum("ebcd,efd->ebcf", grads32, weight32, precision=highest).astype(jnp.bfloat16)
        partial_sum = jnp.einsum("ebcf,ebcd->efd", h32, grads32, precision=highest).astype(jnp.bfloat16)
        partial_sum = lax.optimization_barrier(partial_sum)
        return total + partial_sum.astype(jnp.float32), (mixed, gate_grads, hidden_grads)

    start_total = jnp.zeros((N_EXPERT, F, D), jnp.float32)
    total, stacked = lax.scan(one_row, start_total, (h_all, id_all, gate_all, cot_all))
    mixed, gate_grads, hidden_grads = stacked
    return (mixed.reshape(N_DP * N_EXPERT * TOK_DEV, D), gate_grads.reshape(N_DP * N_EXPERT * TOK_DEV, TOPK), hidden_grads.reshape(N_DP * N_EXPERT * N_EXPERT * CAP, F), total.astype(jnp.bfloat16))
```

```python
import functools

import jax
import jax.numpy as jnp
from jax import lax
from jax.experimental import pallas as pl
from jax.experimental.pallas import tpu as pltpu
from jax.sharding import PartitionSpec as P

MESH = pl.DeviceIdType.MESH
F32 = jnp.float32
BF16 = jnp.bfloat16


def tile_of(size, want):
    while size % want:
        want //= 2
    return want


def kernel(
    nd, ne, chunks,
    hidden, w, ids, gates, cot,
    mixed, gate_grads, hidden_grads, weight_grads,
    wfull, cot_all, meta_send, meta_recv, gg_send, gg_recv,
    ht, gh, ght, z, wg_send1, wg_recv1, wg_send2, wg_recv2, wg_own,
    mx_send1, mx_recv1, mx_send2, mx_recv2, mx_own,
    wy_s, wy_r, wf_s, wf_r, cz_s, cz_r, cf_s, cf_r, me_s, me_r, gg_s, gg_r,
    g1_s, g1_r, g2_s, g2_r, m1_s, m1_r, m2_s, m2_r, loc,
):
    R, N = nd // 2, ne // 2
    rows, D = w.shape
    tok, topk = ids.shape
    F = hidden.shape[1]
    cap = hidden.shape[0] // ne
    T = ne * tok
    a, e = lax.axis_index("dp"), lax.axis_index("expert")
    r, c = a // 2, a % 2
    q, x = e // 2, e % 2
    tile = tile_of(D, 512)

    def to(a2, e2):
        return {"dp": a2, "expert": e2}

    def remote(src, dst, ss, rs, dev):
        return pltpu.make_async_remote_copy(
            src_ref=src, dst_ref=dst, send_sem=ss, recv_sem=rs, device_id=dev, device_id_type=MESH
        )

    barrier = pltpu.get_barrier_semaphore()
    for d in range(1, ne):
        pl.semaphore_signal(barrier, inc=1, device_id=to(a, (e + d) % ne), device_id_type=MESH)
    for d in range(1, R):
        pl.semaphore_signal(barrier, inc=1, device_id=to(((r + d) % R) * 2 + c, e), device_id_type=MESH)
    pl.semaphore_signal(barrier, inc=1, device_id=to(r * 2 + 1 - c, e), device_id_type=MESH)

    own_w = pltpu.make_async_copy(w, wfull.at[pl.ds(pl.multiple_of(a * rows, rows), rows)], loc.at[0])
    own_w.start()
    own_c = pltpu.make_async_copy(cot, cot_all.at[q, x], loc.at[1])
    own_c.start()

    eye = lax.broadcasted_iota(jnp.int32, (tok, tok), 0) == lax.broadcasted_iota(jnp.int32, (tok, tok), 1)
    upper = (
        lax.broadcasted_iota(jnp.int32, (tok, tok), 0) < lax.broadcasted_iota(jnp.int32, (tok, tok), 1)
    ).astype(F32)

    def to_row(col):
        return jnp.sum(jnp.where(eye, col, 0.0), axis=0, keepdims=True)

    def to_col(row):
        return jnp.sum(jnp.where(eye, row, 0.0), axis=1, keepdims=True)

    idf = ids[...].astype(F32)
    gat = gates[...]
    names = lax.broadcasted_iota(jnp.int32, (ne, tok), 0).astype(F32)
    id_rows = [to_row(idf[:, k : k + 1]) for k in range(topk)]
    choose = jnp.zeros((ne, tok), F32)
    gate_t = jnp.zeros((ne, tok), F32)
    for k in range(topk):
        hit = id_rows[k] == names
        choose = choose + jnp.where(hit, 1.0, 0.0)
        gate_t = gate_t + jnp.where(hit, to_row(gat[:, k : k + 1]), 0.0)
    position = jnp.dot(choose.astype(BF16), upper.astype(BF16), preferred_element_type=F32)
    slot_t = jnp.where(choose > 0.0, position, -1.0)
    meta_send[...] = jnp.zeros_like(meta_send)
    gg_send[...] = jnp.zeros_like(gg_send)
    for k in range(ne):
        meta_send[k // 2, k % 2, 0:1, 0:tok] = slot_t[k : k + 1, :]
        meta_send[k // 2, k % 2, 1:2, 0:tok] = gate_t[k : k + 1, :]
    meta_recv[q, x] = meta_send[q, x]

    pl.semaphore_wait(barrier, ne - 1 + R - 1 + 1)

    step = rows // chunks

    def w_rows(block, i):
        return pl.ds(pl.multiple_of(block * rows + i * step, step), step)

    wy, wf, cz, cf, me = {}, {}, {}, {}, {}
    order = sorted(range(1, N), key=lambda d: min(d, N - d))
    for d in range(1, ne):
        o = (e + d) % ne
        me[d] = remote(
            meta_send.at[o // 2, o % 2], meta_recv.at[q, x], me_s.at[d - 1], me_r.at[d - 1], to(a, o)
        )
        me[d].start()
    for i in range(chunks):
        for d in range(1, R):
            wy[d, i] = remote(
                w.at[pl.ds(i * step, step)], wfull.at[w_rows(a, i)],
                wy_s.at[(d - 1) * chunks + i], wy_r.at[(d - 1) * chunks + i],
                to(((r + d) % R) * 2 + c, e),
            )
            wy[d, i].start()
    for d in order:
        cz[d] = remote(
            cot, cot_all.at[q, x], cz_s.at[d - 1], cz_r.at[d - 1], to(a, ((q + d) % N) * 2 + x)
        )
        cz[d].start()
    cf[0] = remote(cot, cot_all.at[q, x], cf_s.at[0], cf_r.at[0], to(a, q * 2 + 1 - x))
    cf[0].start()
    for i in range(chunks):
        wf[0, i] = remote(
            w.at[pl.ds(i * step, step)], wfull.at[w_rows(a, i)],
            wf_s.at[i], wf_r.at[i], to(r * 2 + 1 - c, e),
        )
        wf[0, i].start()

    def forward_cot(d):
        src = (q - d + N) % N
        cz[d].wait_recv()
        cf[d] = remote(
            cot_all.at[src, x], cot_all.at[src, x], cf_s.at[d], cf_r.at[d], to(a, q * 2 + 1 - x)
        )
        cf[d].start()

    def forward_w(i):
        for d in range(1, R):
            block = ((r - d + R) % R) * 2 + c
            wy[d, i].wait_recv()
            wf[d, i] = remote(
                wfull.at[w_rows(block, i)], wfull.at[w_rows(block, i)],
                wf_s.at[d * chunks + i], wf_r.at[d * chunks + i], to(r * 2 + 1 - c, e),
            )
            wf[d, i].start()

    for d in range(1, ne):
        me[d].wait_recv()

    def route(b):
        return meta_recv[b // 2, b % 2, 0:1, 0:tok], meta_recv[b // 2, b % 2, 1:2, 0:tok]

    def placer(slot_row):
        return (lax.broadcasted_iota(jnp.int32, (cap, tok), 0).astype(F32) == slot_row).astype(BF16)

    for b in range(ne):
        slot_row, gate_row = route(b)
        rows_b = lax.dot_general(
            placer(slot_row), hidden[b * cap : (b + 1) * cap, :], (((0,), (0,)), ((), ())),
            preferred_element_type=F32,
        )
        ht[b // 2, b % 2] = rows_b.astype(BF16)
        gh[b // 2, b % 2] = (to_col(gate_row) * rows_b).astype(BF16)
    ght[...] = gh[...].reshape(T, F).astype(F32).T.astype(BF16)

    half = len(order) // 2
    for d in order[:half]:
        forward_cot(d)
    forward_w(0)
    for d in order[half:]:
        forward_cot(d)
    own_c.wait()
    for d in range(N):
        cf[d].wait_recv()

    def grad_block(block, store):
        left = ght[pl.ds(pl.multiple_of(block * rows, rows), rows), :]

        @pl.loop(0, D // tile)
        def _(j):
            cols = pl.ds(pl.multiple_of(j * tile, tile), tile)
            right = cot_all[:, :, :, cols].reshape(T, tile)
            store(cols, jnp.dot(left, right, preferred_element_type=F32))

    g1, g2, m1, m2, gg = {}, {}, {}, {}, {}
    for k in list(range(1, R)) + [0]:
        o = (r + k) % R

        def put1(cols, val, k=k):
            wg_send1[k, :, cols] = val.astype(BF16)

        grad_block(o * 2 + 1 - c, put1)
        g1[k] = remote(
            wg_send1.at[k], wg_recv1.at[k], g1_s.at[k], g1_r.at[k], to(r * 2 + 1 - c, e)
        )
        g1[k].start()
    mid = max(1, chunks // 2)
    for i in range(1, mid):
        forward_w(i)
    for k in range(1, R):
        o = (r + k) % R
        g1[k].wait_recv()

        def put2(cols, val, k=k):
            wg_send2[k - 1, :, cols] = (val + wg_recv1[k, :, cols].astype(F32)).astype(BF16)

        grad_block(o * 2 + c, put2)
        g2[k] = remote(
            wg_send2.at[k - 1], wg_recv2.at[k - 1], g2_s.at[k - 1], g2_r.at[k - 1], to(o * 2 + c, e)
        )
        g2[k].start()
    g1[0].wait_recv()

    def put3(cols, val):
        wg_own[:, cols] = val + wg_recv1[0, :, cols].astype(F32)

    grad_block(r * 2 + c, put3)

    for i in range(mid, chunks):
        forward_w(i)
    own_w.wait()
    for i in range(chunks):
        for d in range(R):
            wf[d, i].wait_recv()

    def out_block(column, store):
        left = gh[:, pl.ds(column, 1)].reshape(N * tok, F)

        @pl.loop(0, D // tile)
        def _(j):
            cols = pl.ds(pl.multiple_of(j * tile, tile), tile)
            val = jnp.dot(left, wfull[:, cols], preferred_element_type=F32)
            store(cols, val.reshape(N, tok, tile))

    def put4(cols, val):
        mx_send1[:, :, cols] = val.astype(BF16)

    out_block(1 - x, put4)
    for k in order + [0]:
        o = (q + k) % N
        m1[k] = remote(
            mx_send1.at[o], mx_recv1.at[o], m1_s.at[k], m1_r.at[k], to(a, q * 2 + 1 - x)
        )
        m1[k].start()

    def put5(cols, val):
        mx_own[:, :, cols] = val

    out_block(x, put5)

    ftile = tile_of(F, 256)
    @pl.loop(0, F // ftile)
    def _(j):
        part = pl.ds(pl.multiple_of(j * ftile, ftile), ftile)
        z[:, part] = lax.dot_general(
            cot_all[...].reshape(T, D), wfull[part, :], (((1,), (1,)), ((), ())),
            preferred_element_type=F32,
        )

    for k in order:
        o = (q + k) % N
        m1[k].wait_recv()
        mx_send2[o] = (mx_own[o] + mx_recv1[o].astype(F32)).astype(BF16)
        m2[k] = remote(
            mx_send2.at[o], mx_recv2.at[q], m2_s.at[k - 1], m2_r.at[k - 1], to(a, o * 2 + x)
        )
        m2[k].start()

    for b in range(ne):
        zb = z[b * tok : (b + 1) * tok, :]
        slot_row, gate_row = route(b)
        gg_col = jnp.sum(ht[b // 2, b % 2].astype(F32) * zb, axis=1, keepdims=True)
        gg_send[b // 2, b % 2, 0:1, 0:tok] = to_row(gg_col)
        scaled = (to_col(gate_row) * zb).astype(BF16)
        hidden_grads[b * cap : (b + 1) * cap, :] = jnp.dot(
            placer(slot_row), scaled, preferred_element_type=F32
        ).astype(BF16)
    for d in range(1, ne):
        o = (e + d) % ne
        gg[d] = remote(
            gg_send.at[o // 2, o % 2], gg_recv.at[q, x], gg_s.at[d - 1], gg_r.at[d - 1], to(a, o)
        )
        gg[d].start()
    gg_recv[q, x] = gg_send[q, x]

    m1[0].wait_recv()
    total = mx_own[q] + mx_recv1[q].astype(F32)
    for k in order:
        m2[k].wait_recv()
        total = total + mx_recv2[(q - k + N) % N].astype(F32)
    mixed[...] = total.astype(BF16)

    for d in range(1, ne):
        gg[d].wait_recv()
    lanes = lax.broadcasted_iota(jnp.int32, (tok, topk), 1)
    result = jnp.zeros((tok, topk), F32)
    for k in range(topk):
        row = jnp.zeros((1, tok), F32)
        for b in range(ne):
            row = row + jnp.where(id_rows[k] == float(b), gg_recv[b // 2, b % 2, 0:1, 0:tok], 0.0)
        result = jnp.where(lanes == k, to_col(row), result)
    gate_grads[...] = result

    for k in range(1, R):
        g2[k].wait_recv()

    @pl.loop(0, D // tile)
    def _(j):
        cols = pl.ds(pl.multiple_of(j * tile, tile), tile)
        val = wg_own[:, cols]
        for k in range(1, R):
            val = val + wg_recv2[k - 1, :, cols].astype(F32)
        weight_grads[:, cols] = val.astype(BF16)

    for group in (wy, wf, cz, cf, me, g1, g2, m1, m2, gg):
        for copy in group.values():
            copy.wait_send()


def fused(hidden, weight_rows, expert_ids, gates, cotangent):
    nd, ne = lax.axis_size("dp"), lax.axis_size("expert")
    rows, D = weight_rows.shape
    tok, topk = expert_ids.shape
    F = hidden.shape[1]
    T, R, N = ne * tok, nd // 2, ne // 2
    chunks = 4
    while rows % (chunks * 16):
        chunks //= 2
    vm = pltpu.VMEM
    sem = lambda n: pltpu.SemaphoreType.DMA((max(n, 1),))
    spec = pl.BlockSpec(memory_space=pltpu.VMEM)
    return pl.pallas_call(
        functools.partial(kernel, nd, ne, chunks),
        out_shape=(
            jax.ShapeDtypeStruct((tok, D), BF16),
            jax.ShapeDtypeStruct((tok, topk), F32),
            jax.ShapeDtypeStruct(hidden.shape, BF16),
            jax.ShapeDtypeStruct((rows, D), BF16),
        ),
        in_specs=[spec] * 5,
        out_specs=(spec,) * 4,
        scratch_shapes=[
            vm((F, D), BF16), vm((N, 2, tok, D), BF16),
            vm((N, 2, 8, 128), F32), vm((N, 2, 8, 128), F32),
            vm((N, 2, 8, 128), F32), vm((N, 2, 8, 128), F32),
            vm((N, 2, tok, F), BF16), vm((N, 2, tok, F), BF16), vm((F, T), BF16), vm((T, F), F32),
            vm((R, rows, D), BF16), vm((R, rows, D), BF16),
            vm((max(R - 1, 1), rows, D), BF16), vm((max(R - 1, 1), rows, D), BF16), vm((rows, D), F32),
            vm((N, tok, D), BF16), vm((N, tok, D), BF16),
            vm((N, tok, D), BF16), vm((N, tok, D), BF16), vm((N, tok, D), F32),
            sem((R - 1) * chunks), sem((R - 1) * chunks), sem(R * chunks), sem(R * chunks),
            sem(N - 1), sem(N - 1), sem(N), sem(N),
            sem(ne - 1), sem(ne - 1), sem(ne - 1), sem(ne - 1),
            sem(R), sem(R), sem(R - 1), sem(R - 1),
            sem(N), sem(N), sem(N - 1), sem(N - 1), sem(2),
        ],
        compiler_params=pltpu.CompilerParams(
            collective_id=0, has_side_effects=True, vmem_limit_bytes=60 * 1024 * 1024
        ),
    )(hidden, weight_rows, expert_ids, gates, cotangent)


def slot_table(expert_ids, experts, capacity):
    flat_ids = expert_ids.reshape(-1)
    choose = (flat_ids[:, None] == jnp.arange(experts, dtype=jnp.int32)[None, :]).astype(jnp.int32)
    earlier = jnp.cumsum(choose, axis=0) - choose
    position = jnp.sum(earlier * choose, axis=1)
    target = flat_ids * capacity + position
    return (target[None, :] == jnp.arange(experts * capacity, dtype=jnp.int32)[:, None]).astype(BF16)


def plain(hidden, weight_rows, expert_ids, gates, cotangent):
    experts = lax.axis_size("expert")
    capacity = hidden.shape[0] // experts
    tok, topk = expert_ids.shape
    width = cotangent.shape[1]
    table = slot_table(expert_ids, experts, capacity)
    weight = lax.all_gather(weight_rows, "dp", axis=0, tiled=True)
    outputs = jnp.dot(hidden, weight, preferred_element_type=F32).astype(BF16)
    back = lax.all_to_all(outputs, "expert", split_axis=0, concat_axis=0, tiled=True)
    picked = lax.dot_general(table, back, (((0,), (0,)), ((), ())), preferred_element_type=F32)
    picked = picked.reshape(tok, topk, width)
    cot32 = cotangent.astype(F32)[:, None, :]
    mixed = jnp.sum(gates[:, :, None] * picked, axis=1).astype(BF16)
    gate_grads = jnp.sum(picked * cot32, axis=2)
    routed = (gates[:, :, None] * cot32).astype(BF16).reshape(-1, width)
    packed = jnp.dot(table, routed, preferred_element_type=F32).astype(BF16)
    grads = lax.all_to_all(packed, "expert", split_axis=0, concat_axis=0, tiled=True)
    hidden_grads = lax.dot_general(
        grads, weight, (((1,), (1,)), ((), ())), preferred_element_type=F32
    ).astype(BF16)
    partial = lax.dot_general(
        hidden, grads, (((0,), (0,)), ((), ())), preferred_element_type=F32
    ).astype(BF16)
    sums = lax.psum_scatter(partial, "dp", scatter_dimension=0, tiled=True)
    return mixed, gate_grads, hidden_grads, sums


def per_device(hidden, w_down, expert_ids, gates, cotangent):
    nd, ne = lax.axis_size("dp"), lax.axis_size("expert")
    rows, width = w_down.shape[1:]
    cap, tok = hidden.shape[0] // ne, expert_ids.shape[0]
    tiled = rows % 16 == 0 and cap % 16 == 0 and tok % 16 == 0 and tok <= 128
    paired = nd % 2 == 0 and ne % 2 == 0
    body = fused if tiled and paired else plain
    mixed, gate_grads, hidden_grads, sums = body(
        hidden, w_down.reshape(rows, width), expert_ids, gates, cotangent
    )
    return mixed, gate_grads, hidden_grads, sums.reshape(1, rows, width)


def solution(mesh):
    split = P(("dp", "expert"), None)
    weights = P("expert", "dp", None)
    return jax.shard_map(
        per_device,
        mesh=mesh,
        in_specs=(split, weights, split, split, split),
        out_specs=(split, split, split, weights),
        check_vma=False,
    )
```

```python
import functools

import jax
import jax.numpy as jnp
from jax import lax
from jax.experimental import pallas as pl
from jax.experimental.pallas import tpu as pltpu
from jax.sharding import PartitionSpec as P

MESH = pl.DeviceIdType.MESH
F32 = jnp.float32
BF16 = jnp.bfloat16


VMEM_BYTES = 67043328


def kernel(
    nd, ne, C,
    hidden_in, w, ids, gates, cot,
    mixed, gate_grads, hidden_grads, weight_grads,
    hidden, wfull, cot_all, meta_send, meta_recv, gg_send, gg_recv,
    ht, gh, ght, z, wg_send1, wg_recv1, wg_send2, wg_recv2, wg_own,
    mx_send1, mx_recv1, mx_send2, mx_recv2, mx_own,
    wy_s, wy_r, wf_s, wf_r, cz_s, cz_r, cf_s, cf_r, me_s, me_r, gg_s, gg_r,
    g1_s, g1_r, g2_s, g2_r, m1_s, m1_r, m2_s, m2_r, lw, lc, lh,
):
    R, N = nd // 2, ne // 2
    rows, D = w.shape
    topk, tok = ids.shape
    F = hidden.shape[1]
    cap = hidden.shape[0] // ne
    T, cw = ne * tok, D // C
    a, e = lax.axis_index("dp"), lax.axis_index("expert")
    r, c = a // 2, a % 2
    q, x = e // 2, e % 2

    def to(a2, e2):
        return {"dp": a2, "expert": e2}

    def remote(src, dst, ss, rs, dev):
        copy = pltpu.make_async_remote_copy(
            src_ref=src, dst_ref=dst, send_sem=ss, recv_sem=rs, device_id=dev, device_id_type=MESH
        )
        copy.start()
        return copy

    def w_rows(block):
        return pl.ds(pl.multiple_of(block * rows, rows), rows)

    def cols(j):
        return slice(j * cw, (j + 1) * cw)

    barrier = pltpu.get_barrier_semaphore()
    for d in range(1, ne):
        pl.semaphore_signal(barrier, inc=1, device_id=to(a, (e + d) % ne), device_id_type=MESH)
    for d in range(1, R):
        pl.semaphore_signal(barrier, inc=1, device_id=to(((r + d) % R) * 2 + c, e), device_id_type=MESH)
    pl.semaphore_signal(barrier, inc=1, device_id=to(r * 2 + 1 - c, e), device_id_type=MESH)
    own_w, own_c = [], []
    for j in range(C):
        own_w.append(pltpu.make_async_copy(w.at[:, cols(j)], wfull.at[j, w_rows(a)], lw.at[j]))
        own_c.append(pltpu.make_async_copy(cot.at[:, cols(j)], cot_all.at[j, q, x], lc.at[j]))
        own_w[j].start()
        own_c[j].start()
    own_h = pltpu.make_async_copy(hidden_in, hidden, lh.at[0])
    own_h.start()

    eye = lax.broadcasted_iota(jnp.int32, (tok, tok), 0) == lax.broadcasted_iota(jnp.int32, (tok, tok), 1)
    upper = (
        lax.broadcasted_iota(jnp.int32, (tok, tok), 0) < lax.broadcasted_iota(jnp.int32, (tok, tok), 1)
    ).astype(F32)

    def to_row(col):
        return jnp.sum(jnp.where(eye, col, 0.0), axis=0, keepdims=True)

    def to_col(row):
        return jnp.sum(jnp.where(eye, row, 0.0), axis=1, keepdims=True)

    idf = ids[...].astype(F32)
    gat = gates[...]
    names = lax.broadcasted_iota(jnp.int32, (ne, tok), 0).astype(F32)
    id_rows = [idf[k : k + 1, :] for k in range(topk)]
    choose = jnp.zeros((ne, tok), F32)
    gate_t = jnp.zeros((ne, tok), F32)
    for k in range(topk):
        hit = id_rows[k] == names
        choose = choose + jnp.where(hit, 1.0, 0.0)
        gate_t = gate_t + jnp.where(hit, gat[k : k + 1, :], 0.0)
    position = jnp.dot(choose.astype(BF16), upper.astype(BF16), preferred_element_type=F32)
    slot_t = jnp.where(choose > 0.0, position, -1.0)
    meta_send[...] = jnp.zeros_like(meta_send)
    gg_send[...] = jnp.zeros_like(gg_send)
    for k in range(ne):
        meta_send[k // 2, k % 2, 0:1, 0:tok] = slot_t[k : k + 1, :]
        meta_send[k // 2, k % 2, 1:2, 0:tok] = gate_t[k : k + 1, :]
    meta_recv[q, x] = meta_send[q, x]

    pl.semaphore_wait(barrier, ne - 1 + R - 1 + 1)

    wy, wf, cz, cf, me, g1, g2, m1, m2, gg = ({} for _ in range(10))
    order = sorted(range(1, N), key=lambda d: min(d, N - d))
    pair_e, pair_d = to(a, q * 2 + 1 - x), to(r * 2 + 1 - c, e)
    for d in range(1, ne):
        o = (e + d) % ne
        me[d] = remote(
            meta_send.at[o // 2, o % 2], meta_recv.at[q, x], me_s.at[d - 1], me_r.at[d - 1], to(a, o)
        )
    for j in range(C):
        own_w[j].wait()
        own_c[j].wait()
        mine = wfull.at[j, w_rows(a)]
        for d in range(1, R):
            wy[d, j] = remote(
                mine, mine, wy_s.at[d - 1, j], wy_r.at[d - 1, j], to(((r + d) % R) * 2 + c, e)
            )
        ours = cot_all.at[j, q, x]
        for d in order:
            cz[d, j] = remote(
                ours, ours, cz_s.at[d - 1, j], cz_r.at[d - 1, j], to(a, ((q + d) % N) * 2 + x)
            )
        cf[0, j] = remote(ours, ours, cf_s.at[0, j], cf_r.at[0, j], pair_e)
        wf[0, j] = remote(mine, mine, wf_s.at[0, j], wf_r.at[0, j], pair_d)

    def forward_cot(j):
        for d in order:
            block = cot_all.at[j, (q - d + N) % N, x]
            cz[d, j].wait_recv()
            cf[d, j] = remote(block, block, cf_s.at[d, j], cf_r.at[d, j], pair_e)

    def forward_w(j):
        for d in range(1, R):
            block = wfull.at[j, w_rows(((r - d + R) % R) * 2 + c)]
            wy[d, j].wait_recv()
            wf[d, j] = remote(block, block, wf_s.at[d, j], wf_r.at[d, j], pair_d)

    own_h.wait()
    for d in range(1, ne):
        me[d].wait_recv()

    def route(b):
        return meta_recv[b // 2, b % 2, 0:1, 0:tok], meta_recv[b // 2, b % 2, 1:2, 0:tok]

    def placer(slot_row):
        return (lax.broadcasted_iota(jnp.int32, (cap, tok), 0).astype(F32) == slot_row).astype(BF16)

    for b in range(ne):
        slot_row, gate_row = route(b)
        rows_b = lax.dot_general(
            placer(slot_row), hidden[b * cap : (b + 1) * cap, :], (((0,), (0,)), ((), ())),
            preferred_element_type=F32,
        )
        ht[b // 2, b % 2] = rows_b.astype(BF16)
        gh[b // 2, b % 2] = (to_col(gate_row) * rows_b).astype(BF16)
    ght[...] = gh[...].reshape(T, F).astype(F32).T.astype(BF16)

    def cot_part(j):
        forward_cot(j)

    def grads_part(j):
        for d in range(N):
            cf[d, j].wait_recv()
        right = cot_all[j].reshape(T, cw)

        def block_of(block):
            return jnp.dot(ght[w_rows(block), :], right, preferred_element_type=F32)

        for k in range(R):
            wg_send1[j, k] = block_of(((r + k) % R) * 2 + 1 - c).astype(BF16)
        g1[j] = remote(wg_send1.at[j], wg_recv1.at[j], g1_s.at[j], g1_r.at[j], pair_d)
        for k in range(R):
            val = block_of(((r + k) % R) * 2 + c)
            if k == 0:
                wg_own[j] = val
            else:
                wg_hold = val
                if k == 1:
                    g1[j].wait_recv()
                wg_send2[j, k - 1] = (wg_hold + wg_recv1[j, k].astype(F32)).astype(BF16)
                g2[k, j] = remote(
                    wg_send2.at[j, k - 1], wg_recv2.at[j, k - 1], g2_s.at[k - 1, j], g2_r.at[k - 1, j],
                    to(((r + k) % R) * 2 + c, e),
                )
        if R == 1:
            g1[j].wait_recv()

    def out_part(j):
        forward_w(j)
        for d in range(R):
            wf[d, j].wait_recv()
        left = gh[:, pl.ds(1 - x, 1)].reshape(N * tok, F)
        val = jnp.dot(left, wfull[j], preferred_element_type=F32)
        mx_send1[j] = val.astype(BF16).reshape(N, tok, cw)
        m1[j] = remote(mx_send1.at[j], mx_recv1.at[j], m1_s.at[j], m1_r.at[j], pair_e)
        left = gh[:, pl.ds(x, 1)].reshape(N * tok, F)
        val = jnp.dot(left, wfull[j], preferred_element_type=F32)
        mx_own[j] = val.reshape(N, tok, cw)

    def z_part(j):
        val = lax.dot_general(
            cot_all[j].reshape(T, cw), wfull[j], (((1,), (1,)), ((), ())), preferred_element_type=F32
        )
        z[...] = val if j == 0 else z[...] + val

    def mix_part(j):
        m1[j].wait_recv()
        for k in order:
            o = (q + k) % N
            mx_send2[j, o] = (mx_own[j, o] + mx_recv1[j, o].astype(F32)).astype(BF16)
            m2[k, j] = remote(
                mx_send2.at[j, o], mx_recv2.at[j, q], m2_s.at[k - 1, j], m2_r.at[k - 1, j],
                to(a, o * 2 + x),
            )

    cot_part(0)
    for j in range(C):
        if j + 1 < C:
            cot_part(j + 1)
        out_part(j)
        grads_part(j)
        z_part(j)
        if j > 0:
            mix_part(j - 1)
    mix_part(C - 1)

    for b in range(ne):
        zb = z[b * tok : (b + 1) * tok, :]
        slot_row, gate_row = route(b)
        gg_col = jnp.sum(ht[b // 2, b % 2].astype(F32) * zb, axis=1, keepdims=True)
        gg_send[b // 2, b % 2, 0:1, 0:tok] = to_row(gg_col)
        scaled = (to_col(gate_row) * zb).astype(BF16)
        hidden_grads[b * cap : (b + 1) * cap, :] = jnp.dot(
            placer(slot_row), scaled, preferred_element_type=F32
        ).astype(BF16)
    for d in range(1, ne):
        o = (e + d) % ne
        gg[d] = remote(
            gg_send.at[o // 2, o % 2], gg_recv.at[q, x], gg_s.at[d - 1], gg_r.at[d - 1], to(a, o)
        )
    gg_recv[q, x] = gg_send[q, x]

    for j in range(C):
        total = mx_own[j, q] + mx_recv1[j, q].astype(F32)
        for k in order:
            m2[k, j].wait_recv()
            total = total + mx_recv2[j, (q - k + N) % N].astype(F32)
        mixed[:, cols(j)] = total.astype(BF16)

    for d in range(1, ne):
        gg[d].wait_recv()
    for k in range(topk):
        row = jnp.zeros((1, tok), F32)
        for b in range(ne):
            row = row + jnp.where(id_rows[k] == float(b), gg_recv[b // 2, b % 2, 0:1, 0:tok], 0.0)
        gate_grads[k : k + 1, :] = row

    for j in range(C):
        val = wg_own[j] + wg_recv1[j, 0].astype(F32)
        for k in range(1, R):
            g2[k, j].wait_recv()
            val = val + wg_recv2[j, k - 1].astype(F32)
        weight_grads[:, cols(j)] = val.astype(BF16)

    for group in (wy, wf, cz, cf, me, g1, g2, m1, m2, gg):
        for copy in group.values():
            copy.wait_send()


def store_kernel(count, *refs):
    sems = refs[-1]
    copies = [pltpu.make_async_copy(refs[i], refs[count + i], sems.at[i]) for i in range(count)]
    for copy in copies:
        copy.start()
    for copy in copies:
        copy.wait()


def fused(hidden, weight_rows, expert_ids, gates, cotangent):
    nd, ne = lax.axis_size("dp"), lax.axis_size("expert")
    rows, D = weight_rows.shape
    tok, topk = expert_ids.shape
    F = hidden.shape[1]
    T, R, N = ne * tok, nd // 2, ne // 2
    C = 4
    while D % (C * 128):
        C //= 2
    cw = D // C
    vm = pltpu.VMEM
    sem = lambda *n: pltpu.SemaphoreType.DMA(tuple(max(i, 1) for i in n))
    near, far = pl.BlockSpec(memory_space=pltpu.VMEM), pl.BlockSpec(memory_space=pltpu.HBM)
    shapes = [((tok, D), BF16), ((topk, tok), F32), (hidden.shape, BF16), ((rows, D), BF16)]
    last = max(R - 1, 1)
    result_bytes = 2 * (tok * D + hidden.size + rows * D) + 128 * 1024
    results = pl.pallas_call(
        functools.partial(kernel, nd, ne, C),
        out_shape=tuple(pltpu.VMEM(*s) for s in shapes),
        in_specs=[far, far, near, near, far],
        out_specs=(near,) * 4,
        scratch_shapes=[
            vm(hidden.shape, BF16), vm((C, F, cw), BF16), vm((C, N, 2, tok, cw), BF16),
            vm((N, 2, 8, 128), F32), vm((N, 2, 8, 128), F32),
            vm((N, 2, 8, 128), F32), vm((N, 2, 8, 128), F32),
            vm((N, 2, tok, F), BF16), vm((N, 2, tok, F), BF16), vm((F, T), BF16), vm((T, F), F32),
            vm((C, R, rows, cw), BF16), vm((C, R, rows, cw), BF16),
            vm((C, last, rows, cw), BF16), vm((C, last, rows, cw), BF16), vm((C, rows, cw), F32),
            vm((C, N, tok, cw), BF16), vm((C, N, tok, cw), BF16),
            vm((C, N, tok, cw), BF16), vm((C, N, tok, cw), BF16), vm((C, N, tok, cw), F32),
            sem(R - 1, C), sem(R - 1, C), sem(R, C), sem(R, C),
            sem(N - 1, C), sem(N - 1, C), sem(N, C), sem(N, C),
            sem(ne - 1), sem(ne - 1), sem(ne - 1), sem(ne - 1),
            sem(C), sem(C), sem(R - 1, C), sem(R - 1, C),
            sem(C), sem(C), sem(N - 1, C), sem(N - 1, C), sem(C), sem(C), sem(1),
        ],
        compiler_params=pltpu.CompilerParams(
            collective_id=0, has_side_effects=True, vmem_limit_bytes=VMEM_BYTES - result_bytes
        ),
    )(hidden, weight_rows, expert_ids.T, gates.T, cotangent)
    mixed, gate_grads, hidden_grads, sums = pl.pallas_call(
        functools.partial(store_kernel, len(shapes)),
        out_shape=tuple(jax.ShapeDtypeStruct(*s) for s in shapes),
        in_specs=[pl.BlockSpec(memory_space=pl.ANY)] * 4,
        out_specs=(far,) * 4,
        scratch_shapes=[sem(len(shapes))],
        compiler_params=pltpu.CompilerParams(vmem_limit_bytes=1024 * 1024),
    )(*results)
    return mixed, gate_grads.T, hidden_grads, sums


def slot_table(expert_ids, experts, capacity):
    flat_ids = expert_ids.reshape(-1)
    choose = (flat_ids[:, None] == jnp.arange(experts, dtype=jnp.int32)[None, :]).astype(jnp.int32)
    earlier = jnp.cumsum(choose, axis=0) - choose
    position = jnp.sum(earlier * choose, axis=1)
    target = flat_ids * capacity + position
    return (target[None, :] == jnp.arange(experts * capacity, dtype=jnp.int32)[:, None]).astype(BF16)


def plain(hidden, weight_rows, expert_ids, gates, cotangent):
    experts = lax.axis_size("expert")
    capacity = hidden.shape[0] // experts
    tok, topk = expert_ids.shape
    width = cotangent.shape[1]
    table = slot_table(expert_ids, experts, capacity)
    weight = lax.all_gather(weight_rows, "dp", axis=0, tiled=True)
    outputs = jnp.dot(hidden, weight, preferred_element_type=F32).astype(BF16)
    back = lax.all_to_all(outputs, "expert", split_axis=0, concat_axis=0, tiled=True)
    picked = lax.dot_general(table, back, (((0,), (0,)), ((), ())), preferred_element_type=F32)
    picked = picked.reshape(tok, topk, width)
    cot32 = cotangent.astype(F32)[:, None, :]
    mixed = jnp.sum(gates[:, :, None] * picked, axis=1).astype(BF16)
    gate_grads = jnp.sum(picked * cot32, axis=2)
    routed = (gates[:, :, None] * cot32).astype(BF16).reshape(-1, width)
    packed = jnp.dot(table, routed, preferred_element_type=F32).astype(BF16)
    grads = lax.all_to_all(packed, "expert", split_axis=0, concat_axis=0, tiled=True)
    hidden_grads = lax.dot_general(
        grads, weight, (((1,), (1,)), ((), ())), preferred_element_type=F32
    ).astype(BF16)
    partial = lax.dot_general(
        hidden, grads, (((0,), (0,)), ((), ())), preferred_element_type=F32
    ).astype(BF16)
    sums = lax.psum_scatter(partial, "dp", scatter_dimension=0, tiled=True)
    return mixed, gate_grads, hidden_grads, sums


def per_device(hidden, w_down, expert_ids, gates, cotangent):
    nd, ne = lax.axis_size("dp"), lax.axis_size("expert")
    rows, width = w_down.shape[1:]
    cap, tok = hidden.shape[0] // ne, expert_ids.shape[0]
    tiled = rows % 16 == 0 and cap % 16 == 0 and tok % 16 == 0 and tok <= 128
    paired = nd % 2 == 0 and ne % 2 == 0
    body = fused if tiled and paired else plain
    mixed, gate_grads, hidden_grads, sums = body(
        hidden, w_down.reshape(rows, width), expert_ids, gates, cotangent
    )
    return mixed, gate_grads, hidden_grads, sums.reshape(1, rows, width)


def solution(mesh):
    split = P(("dp", "expert"), None)
    weights = P("expert", "dp", None)
    return jax.shard_map(
        per_device,
        mesh=mesh,
        in_specs=(split, weights, split, split, split),
        out_specs=(split, split, split, weights),
        check_vma=False,
    )
```

```python
import functools

import jax
import jax.numpy as jnp
from jax import lax
from jax.experimental import pallas as pl
from jax.experimental.pallas import tpu as pltpu
from jax.sharding import PartitionSpec as P

MESH = pl.DeviceIdType.MESH
F32 = jnp.float32
BF16 = jnp.bfloat16


VMEM_BYTES = 67043328


def kernel(
    nd, ne, C,
    hidden_in, w, ids, gates, cot,
    mixed, gate_grads, hidden_grads, weight_grads,
    hidden, wfull, cot_all, meta, gg_send, gg_recv,
    ht, gh, ght, z, wg_send1, wg_recv1, wg_send2, wg_recv2, wg_own,
    mx_send1, mx_recv1, mx_send2, mx_recv2, mx_own,
    wy_s, wy_r, wf_s, wf_r, cz_s, cz_r, cf_s, cf_r, gg_s, gg_r,
    g1_s, g1_r, g2_s, g2_r, m1_s, m1_r, m2_s, m2_r, lw, lc, lh,
):
    R, N = nd // 2, ne // 2
    rows, D = w.shape
    topk, tok = ids.shape
    F = hidden.shape[1]
    cap = hidden.shape[0] // ne
    T, cw = ne * tok, D // C
    a, e = lax.axis_index("dp"), lax.axis_index("expert")
    r, c = a // 2, a % 2
    q, x = e // 2, e % 2

    def to(a2, e2):
        return {"dp": a2, "expert": e2}

    def remote(src, dst, ss, rs, dev):
        copy = pltpu.make_async_remote_copy(
            src_ref=src, dst_ref=dst, send_sem=ss, recv_sem=rs, device_id=dev, device_id_type=MESH
        )
        copy.start()
        return copy

    def w_rows(block):
        return pl.ds(pl.multiple_of(block * rows, rows), rows)

    def cols(j):
        return slice(j * cw, (j + 1) * cw)

    barrier = pltpu.get_barrier_semaphore()
    pl.semaphore_signal(barrier, inc=1, device_id=to(a, q * 2 + 1 - x), device_id_type=MESH)

    @pl.when(q > 0)
    def _():
        pl.semaphore_signal(barrier, inc=1, device_id=to(a, (q - 1) * 2 + x), device_id_type=MESH)

    @pl.when(q < N - 1)
    def _():
        pl.semaphore_signal(barrier, inc=1, device_id=to(a, (q + 1) * 2 + x), device_id_type=MESH)

    for d in range(1, R):
        pl.semaphore_signal(barrier, inc=1, device_id=to(((r + d) % R) * 2 + c, e), device_id_type=MESH)
    pl.semaphore_signal(barrier, inc=1, device_id=to(r * 2 + 1 - c, e), device_id_type=MESH)
    own_w, own_c = [], []
    for j in range(C):
        own_w.append(pltpu.make_async_copy(w.at[:, cols(j)], wfull.at[j, w_rows(a)], lw.at[j]))
        own_c.append(pltpu.make_async_copy(cot.at[:, cols(j)], cot_all.at[j, q, x], lc.at[j]))
        own_w[j].start()
        own_c[j].start()
    own_h = pltpu.make_async_copy(hidden_in, hidden, lh.at[0])
    own_h.start()

    eye = lax.broadcasted_iota(jnp.int32, (tok, tok), 0) == lax.broadcasted_iota(jnp.int32, (tok, tok), 1)
    upper = (
        lax.broadcasted_iota(jnp.int32, (tok, tok), 0) < lax.broadcasted_iota(jnp.int32, (tok, tok), 1)
    ).astype(F32)

    def to_row(col):
        return jnp.sum(jnp.where(eye, col, 0.0), axis=0, keepdims=True)

    def to_col(row):
        return jnp.sum(jnp.where(eye, row, 0.0), axis=1, keepdims=True)

    idf = ids[...].astype(F32)
    gat = gates[...]
    names = lax.broadcasted_iota(jnp.int32, (ne, tok), 0).astype(F32)
    id_rows = [idf[k : k + 1, :] for k in range(topk)]
    choose = jnp.zeros((ne, tok), F32)
    gate_t = jnp.zeros((ne, tok), F32)
    for k in range(topk):
        hit = id_rows[k] == names
        choose = choose + jnp.where(hit, 1.0, 0.0)
        gate_t = gate_t + jnp.where(hit, gat[k : k + 1, :], 0.0)
    position = jnp.dot(choose.astype(BF16), upper.astype(BF16), preferred_element_type=F32)
    slot_t = jnp.where(choose > 0.0, position, -1.0)
    meta[q, x] = jnp.zeros((2 * ne, 128), F32)
    gg_send[...] = jnp.zeros_like(gg_send)
    meta[q, x, 0:ne, 0:tok] = slot_t
    meta[q, x, ne : 2 * ne, 0:tok] = gate_t

    pl.semaphore_wait(barrier, R + 1 + (q + N - 1) // N + (2 * N - 2 - q) // N)

    wy, wf, g1, g2, m1, m2, gg = ({} for _ in range(7))
    order = sorted(range(1, N), key=lambda d: min(d, N - d))
    pair_e, pair_d = to(a, q * 2 + 1 - x), to(r * 2 + 1 - c, e)

    def piece(j, i, column):
        return cot_all.at[j, i, column] if j < C else meta.at[i, column]

    def hop(j, s, i, side):
        way = 1 if side == 0 else -1
        return pltpu.make_async_remote_copy(
            src_ref=piece(j, i, x), dst_ref=piece(j, i, x), send_sem=cz_s.at[side, s - 1, j],
            recv_sem=cz_r.at[side, s - 1, j], device_id=to(a, (q + way) * 2 + x), device_id_type=MESH,
        )

    def cross(j, i, column):
        return pltpu.make_async_remote_copy(
            src_ref=piece(j, i, column), dst_ref=piece(j, i, column), send_sem=cf_s.at[i, j],
            recv_sem=cf_r.at[i, j], device_id=pair_e, device_id_type=MESH,
        )

    def each_hop(act):
        for side in range(2):
            ahead = q < N - 1 if side == 0 else q > 0
            for s in range(1, N):
                held = q >= s - 1 if side == 0 else q + s - 1 < N

                @pl.when(jnp.logical_and(ahead, held))
                def _(side=side, s=s):
                    act(s, q - s + 1 if side == 0 else q + s - 1, side)

    def begin(j):
        @pl.when(q < N - 1)
        def _():
            hop(j, 1, q, 0).start()

        @pl.when(q > 0)
        def _():
            hop(j, 1, q, 1).start()

        cross(j, q, x).start()

    def relay(s):
        for j in [C] + list(range(C)):
            for side in range(2):
                there = q >= s if side == 0 else q + s < N
                onward = q < N - 1 if side == 0 else q > 0
                i = q - s if side == 0 else q + s

                @pl.when(there)
                def _(j=j, side=side, i=i, onward=onward):
                    hop(j, s, i, side).wait_recv()
                    if s < N - 1:

                        @pl.when(onward)
                        def _():
                            hop(j, s + 1, i, side).start()

                    cross(j, i, x).start()

    begin(C)
    for j in range(C):
        own_w[j].wait()
        own_c[j].wait()
        mine = wfull.at[j, w_rows(a)]
        for d in range(1, R):
            wy[d, j] = remote(
                mine, mine, wy_s.at[d - 1, j], wy_r.at[d - 1, j], to(((r + d) % R) * 2 + c, e)
            )
        begin(j)
        wf[0, j] = remote(mine, mine, wf_s.at[0, j], wf_r.at[0, j], pair_d)

    def forward_w(j):
        for d in range(1, R):
            block = wfull.at[j, w_rows(((r - d + R) % R) * 2 + c)]
            wy[d, j].wait_recv()
            wf[d, j] = remote(block, block, wf_s.at[d, j], wf_r.at[d, j], pair_d)

    own_h.wait()
    for s in range(1, N):
        relay(s)
    for i in range(N):
        cross(C, i, 1 - x).wait_recv()

    def route(b):
        slot_row = meta[b // 2, b % 2, pl.ds(e, 1), :]
        gate_row = meta[b // 2, b % 2, pl.ds(ne + e, 1), :]
        return slot_row[:, 0:tok], gate_row[:, 0:tok]

    def placer(slot_row):
        return (lax.broadcasted_iota(jnp.int32, (cap, tok), 0).astype(F32) == slot_row).astype(BF16)

    for b in range(ne):
        slot_row, gate_row = route(b)
        rows_b = lax.dot_general(
            placer(slot_row), hidden[b * cap : (b + 1) * cap, :], (((0,), (0,)), ((), ())),
            preferred_element_type=F32,
        )
        ht[b // 2, b % 2] = rows_b.astype(BF16)
        gh[b // 2, b % 2] = (to_col(gate_row) * rows_b).astype(BF16)
    ght[...] = gh[...].reshape(T, F).astype(F32).T.astype(BF16)

    def grads_part(j):
        for i in range(N):
            cross(j, i, 1 - x).wait_recv()
        right = cot_all[j].reshape(T, cw)

        def block_of(block):
            return jnp.dot(ght[w_rows(block), :], right, preferred_element_type=F32)

        for k in range(R):
            wg_send1[j, k] = block_of(((r + k) % R) * 2 + 1 - c).astype(BF16)
        g1[j] = remote(wg_send1.at[j], wg_recv1.at[j], g1_s.at[j], g1_r.at[j], pair_d)
        for k in range(R):
            val = block_of(((r + k) % R) * 2 + c)
            if k == 0:
                wg_own[j] = val
            else:
                wg_hold = val
                if k == 1:
                    g1[j].wait_recv()
                wg_send2[j, k - 1] = (wg_hold + wg_recv1[j, k].astype(F32)).astype(BF16)
                g2[k, j] = remote(
                    wg_send2.at[j, k - 1], wg_recv2.at[j, k - 1], g2_s.at[k - 1, j], g2_r.at[k - 1, j],
                    to(((r + k) % R) * 2 + c, e),
                )
        if R == 1:
            g1[j].wait_recv()

    def out_part(j):
        forward_w(j)
        for d in range(R):
            wf[d, j].wait_recv()
        left = gh[:, pl.ds(1 - x, 1)].reshape(N * tok, F)
        val = jnp.dot(left, wfull[j], preferred_element_type=F32)
        mx_send1[j] = val.astype(BF16).reshape(N, tok, cw)
        m1[j] = remote(mx_send1.at[j], mx_recv1.at[j], m1_s.at[j], m1_r.at[j], pair_e)
        left = gh[:, pl.ds(x, 1)].reshape(N * tok, F)
        val = jnp.dot(left, wfull[j], preferred_element_type=F32)
        mx_own[j] = val.reshape(N, tok, cw)

    def z_part(j):
        val = lax.dot_general(
            cot_all[j].reshape(T, cw), wfull[j], (((1,), (1,)), ((), ())), preferred_element_type=F32
        )
        z[...] = val if j == 0 else z[...] + val

    def mix_part(j):
        m1[j].wait_recv()
        for k in order:
            o = (q + k) % N
            mx_send2[j, o] = (mx_own[j, o] + mx_recv1[j, o].astype(F32)).astype(BF16)
            m2[k, j] = remote(
                mx_send2.at[j, o], mx_recv2.at[j, q], m2_s.at[k - 1, j], m2_r.at[k - 1, j],
                to(a, o * 2 + x),
            )

    for j in range(C):
        out_part(j)
        grads_part(j)
        z_part(j)
        if j > 0:
            mix_part(j - 1)
    mix_part(C - 1)

    for b in range(ne):
        zb = z[b * tok : (b + 1) * tok, :]
        slot_row, gate_row = route(b)
        gg_col = jnp.sum(ht[b // 2, b % 2].astype(F32) * zb, axis=1, keepdims=True)
        gg_send[b // 2, b % 2, 0:1, 0:tok] = to_row(gg_col)
        scaled = (to_col(gate_row) * zb).astype(BF16)
        hidden_grads[b * cap : (b + 1) * cap, :] = jnp.dot(
            placer(slot_row), scaled, preferred_element_type=F32
        ).astype(BF16)
    for d in range(1, ne):
        o = (e + d) % ne
        gg[d] = remote(
            gg_send.at[o // 2, o % 2], gg_recv.at[q, x], gg_s.at[d - 1], gg_r.at[d - 1], to(a, o)
        )
    gg_recv[q, x] = gg_send[q, x]

    for j in range(C):
        total = mx_own[j, q] + mx_recv1[j, q].astype(F32)
        for k in order:
            m2[k, j].wait_recv()
            total = total + mx_recv2[j, (q - k + N) % N].astype(F32)
        mixed[:, cols(j)] = total.astype(BF16)

    for d in range(1, ne):
        gg[d].wait_recv()
    for k in range(topk):
        row = jnp.zeros((1, tok), F32)
        for b in range(ne):
            row = row + jnp.where(id_rows[k] == float(b), gg_recv[b // 2, b % 2, 0:1, 0:tok], 0.0)
        gate_grads[k : k + 1, :] = row

    for j in range(C):
        val = wg_own[j] + wg_recv1[j, 0].astype(F32)
        for k in range(1, R):
            g2[k, j].wait_recv()
            val = val + wg_recv2[j, k - 1].astype(F32)
        weight_grads[:, cols(j)] = val.astype(BF16)

    for group in (wy, wf, g1, g2, m1, m2, gg):
        for copy in group.values():
            copy.wait_send()
    for j in range(C + 1):
        each_hop(lambda s, i, side, j=j: hop(j, s, i, side).wait_send())
        for i in range(N):
            cross(j, i, x).wait_send()


def store_kernel(count, *refs):
    sems = refs[-1]
    copies = [pltpu.make_async_copy(refs[i], refs[count + i], sems.at[i]) for i in range(count)]
    for copy in copies:
        copy.start()
    for copy in copies:
        copy.wait()


def fused(hidden, weight_rows, expert_ids, gates, cotangent):
    nd, ne = lax.axis_size("dp"), lax.axis_size("expert")
    rows, D = weight_rows.shape
    tok, topk = expert_ids.shape
    F = hidden.shape[1]
    T, R, N = ne * tok, nd // 2, ne // 2
    C = 4
    while D % (C * 128):
        C //= 2
    cw = D // C
    vm = pltpu.VMEM
    sem = lambda *n: pltpu.SemaphoreType.DMA(tuple(max(i, 1) for i in n))
    near, far = pl.BlockSpec(memory_space=pltpu.VMEM), pl.BlockSpec(memory_space=pltpu.HBM)
    shapes = [((tok, D), BF16), ((topk, tok), F32), (hidden.shape, BF16), ((rows, D), BF16)]
    last = max(R - 1, 1)
    result_bytes = 2 * (tok * D + hidden.size + rows * D) + 128 * 1024
    results = pl.pallas_call(
        functools.partial(kernel, nd, ne, C),
        out_shape=tuple(pltpu.VMEM(*s) for s in shapes),
        in_specs=[far, far, near, near, far],
        out_specs=(near,) * 4,
        scratch_shapes=[
            vm(hidden.shape, BF16), vm((C, F, cw), BF16), vm((C, N, 2, tok, cw), BF16),
            vm((N, 2, 2 * ne, 128), F32), vm((N, 2, 8, 128), F32), vm((N, 2, 8, 128), F32),
            vm((N, 2, tok, F), BF16), vm((N, 2, tok, F), BF16), vm((F, T), BF16), vm((T, F), F32),
            vm((C, R, rows, cw), BF16), vm((C, R, rows, cw), BF16),
            vm((C, last, rows, cw), BF16), vm((C, last, rows, cw), BF16), vm((C, rows, cw), F32),
            vm((C, N, tok, cw), BF16), vm((C, N, tok, cw), BF16),
            vm((C, N, tok, cw), BF16), vm((C, N, tok, cw), BF16), vm((C, N, tok, cw), F32),
            sem(R - 1, C), sem(R - 1, C), sem(R, C), sem(R, C),
            sem(2, N - 1, C + 1), sem(2, N - 1, C + 1), sem(N, C + 1), sem(N, C + 1),
            sem(ne - 1), sem(ne - 1),
            sem(C), sem(C), sem(R - 1, C), sem(R - 1, C),
            sem(C), sem(C), sem(N - 1, C), sem(N - 1, C), sem(C), sem(C), sem(1),
        ],
        compiler_params=pltpu.CompilerParams(
            collective_id=0, has_side_effects=True, vmem_limit_bytes=VMEM_BYTES - result_bytes
        ),
    )(hidden, weight_rows, expert_ids.T, gates.T, cotangent)
    mixed, gate_grads, hidden_grads, sums = pl.pallas_call(
        functools.partial(store_kernel, len(shapes)),
        out_shape=tuple(jax.ShapeDtypeStruct(*s) for s in shapes),
        in_specs=[pl.BlockSpec(memory_space=pl.ANY)] * 4,
        out_specs=(far,) * 4,
        scratch_shapes=[sem(len(shapes))],
        compiler_params=pltpu.CompilerParams(vmem_limit_bytes=1024 * 1024),
    )(*results)
    return mixed, gate_grads.T, hidden_grads, sums


def slot_table(expert_ids, experts, capacity):
    flat_ids = expert_ids.reshape(-1)
    choose = (flat_ids[:, None] == jnp.arange(experts, dtype=jnp.int32)[None, :]).astype(jnp.int32)
    earlier = jnp.cumsum(choose, axis=0) - choose
    position = jnp.sum(earlier * choose, axis=1)
    target = flat_ids * capacity + position
    return (target[None, :] == jnp.arange(experts * capacity, dtype=jnp.int32)[:, None]).astype(BF16)


def plain(hidden, weight_rows, expert_ids, gates, cotangent):
    experts = lax.axis_size("expert")
    capacity = hidden.shape[0] // experts
    tok, topk = expert_ids.shape
    width = cotangent.shape[1]
    table = slot_table(expert_ids, experts, capacity)
    weight = lax.all_gather(weight_rows, "dp", axis=0, tiled=True)
    outputs = jnp.dot(hidden, weight, preferred_element_type=F32).astype(BF16)
    back = lax.all_to_all(outputs, "expert", split_axis=0, concat_axis=0, tiled=True)
    picked = lax.dot_general(table, back, (((0,), (0,)), ((), ())), preferred_element_type=F32)
    picked = picked.reshape(tok, topk, width)
    cot32 = cotangent.astype(F32)[:, None, :]
    mixed = jnp.sum(gates[:, :, None] * picked, axis=1).astype(BF16)
    gate_grads = jnp.sum(picked * cot32, axis=2)
    routed = (gates[:, :, None] * cot32).astype(BF16).reshape(-1, width)
    packed = jnp.dot(table, routed, preferred_element_type=F32).astype(BF16)
    grads = lax.all_to_all(packed, "expert", split_axis=0, concat_axis=0, tiled=True)
    hidden_grads = lax.dot_general(
        grads, weight, (((1,), (1,)), ((), ())), preferred_element_type=F32
    ).astype(BF16)
    partial = lax.dot_general(
        hidden, grads, (((0,), (0,)), ((), ())), preferred_element_type=F32
    ).astype(BF16)
    sums = lax.psum_scatter(partial, "dp", scatter_dimension=0, tiled=True)
    return mixed, gate_grads, hidden_grads, sums


def per_device(hidden, w_down, expert_ids, gates, cotangent):
    nd, ne = lax.axis_size("dp"), lax.axis_size("expert")
    rows, width = w_down.shape[1:]
    cap, tok = hidden.shape[0] // ne, expert_ids.shape[0]
    tiled = rows % 16 == 0 and cap % 16 == 0 and tok % 16 == 0 and tok <= 128
    paired = nd % 2 == 0 and ne % 2 == 0
    body = fused if tiled and paired else plain
    mixed, gate_grads, hidden_grads, sums = body(
        hidden, w_down.reshape(rows, width), expert_ids, gates, cotangent
    )
    return mixed, gate_grads, hidden_grads, sums.reshape(1, rows, width)


def solution(mesh):
    split = P(("dp", "expert"), None)
    weights = P("expert", "dp", None)
    return jax.shard_map(
        per_device,
        mesh=mesh,
        in_specs=(split, weights, split, split, split),
        out_specs=(split, split, split, weights),
        check_vma=False,
    )
```
